32 devices in a mesh: blk: 16 (over z, y, x), band: 2 (over core).
Axes of the slice: x: 2, y: 2, z: 4, core: 2. Of those that a mesh axis runs over, the one named last changes fastest.
Arguments:
- disp_fwd: float32 [16, 2, 25, 2048], P('blk', 'band'), may hold values from -6 to 6
- prev_fwd: float32 [16, 2, 25, 2048], P('blk', 'band'), may hold values from -6 to 6
- disp_adj: float32 [16, 2, 25, 2048], P('blk', 'band'), may hold values from -6 to 6
- prev_adj: float32 [16, 2, 25, 2048], P('blk', 'band'), may hold values from -6 to 6
- modulus: float32 [16, 2, 25, 2048], P('blk', 'band'), may hold values from 0.5 to 2
- radius: float32 [16, 2, 25], P('blk', 'band'), may hold values from 256 to 2048
- step_scale: float32 [16, 2, 25], P('blk', 'band'), may hold values from 0.01 to 0.04
- kernel_in: float32 [16, 2, 25, 2048], P('blk', 'band'), may hold values from -6 to 6
- buckets: int32 [16, 2], P('blk', 'band'), may hold values from 0 to 3
- halo_count: int32 [16, 2, 4], P('blk', 'band'), may hold values from 0 to 8, as said below
- blk_nodes: int32 [16, 2, 2, 8], P('blk', 'band'), may hold values from 0 to 24, as said below
- band_nodes: int32 [16, 2, 2, 4], P('blk', 'band'), may hold values from 0 to 24, as said below
Outputs:
- next_fwd: float32 [16, 2, 25, 2048], P('blk', 'band')
- next_adj: float32 [16, 2, 25, 2048], P('blk', 'band')
- kernel_out: float32 [16, 2, 25, 2048], P('blk', 'band')
The draws below stay inside these ranges and needn't reach their ends.
Inputs may be any that keep to these rules, and one draw needn't show every extreme that they name: `halo_count`: entries 0 and 1 count the nodes shared with the blk neighbour below and above, entries 2 and 3 with the band neighbour below and above. A device's count toward a neighbour equals the neighbour's count back; counts toward the outside of the grid are zero; some pair along blk shares 8 nodes and some pair along band 4. Slot k of a device's list toward a blk neighbour and slot k of that neighbour's list back hold copies of one node; slots at or past the count are unused. The 24 ids of one device over blk_nodes and band_nodes are all different. `band_nodes`: slot k of a device's list toward a band neighbour and slot k of that neighbour's list back hold copies of one node; slots at or past the count are unused; ids are different from those of blk_nodes on the same device.
All inputs are finite; a program needn't handle non-finite values.
Results may differ from the reference program's by a relative error of at most 0.0046.
Values sent between devices are 32-bit elements; how exact they have to be, the bound alone decides.
A program may use at most 64 MiB of HBM per device.

```python
import math
import jax
import jax.numpy as jnp
import numpy as np
from jax import lax

MODES = 1024
COEFF = 2048
SAMPLES = 2048
NODES = 25
EL_DEV = 1
SHARED_Z = 4
SHARED_B = 8
GRID_B = 16
GRID_Z = 2
DEPTH = 2


def shuffle(single_key):
    return jax.random.permutation(single_key, EL_DEV * NODES).astype(jnp.int32)


def halo_plan(key):
    blk_key = jax.random.fold_in(key, 101)
    band_key = jax.random.fold_in(key, 202)
    counts_blk = jax.random.randint(jax.random.fold_in(blk_key, 1), (GRID_B - 1, GRID_Z), 1, SHARED_B + 1, dtype=jnp.int32)
    forced_blk = jax.random.randint(jax.random.fold_in(blk_key, 2), (), 0, (GRID_B - 1) * GRID_Z, dtype=jnp.int32)
    counts_blk = counts_blk.reshape(-1).at[forced_blk].set(SHARED_B).reshape(GRID_B - 1, GRID_Z)
    counts_band = jax.random.randint(jax.random.fold_in(band_key, 1), (GRID_B, GRID_Z - 1), 1, SHARED_Z + 1, dtype=jnp.int32)
    forced_band = jax.random.randint(jax.random.fold_in(band_key, 2), (), 0, GRID_B * (GRID_Z - 1), dtype=jnp.int32)
    counts_band = counts_band.reshape(-1).at[forced_band].set(SHARED_Z).reshape(GRID_B, GRID_Z - 1)
    zero_row = jnp.zeros((1, GRID_Z), jnp.int32)
    zero_col = jnp.zeros((GRID_B, 1), jnp.int32)
    lower_blk = jnp.concatenate([zero_row, counts_blk], axis=0)
    upper_blk = jnp.concatenate([counts_blk, zero_row], axis=0)
    lower_band = jnp.concatenate([zero_col, counts_band], axis=1)
    upper_band = jnp.concatenate([counts_band, zero_col], axis=1)
    counts = jnp.stack([lower_blk, upper_blk, lower_band, upper_band], axis=-1)
    perm_keys = jax.random.split(jax.random.fold_in(key, 303), GRID_B * GRID_Z)
    shuffled = jax.vmap(shuffle)(perm_keys)
    blk_lists = shuffled[:, :2 * SHARED_B].reshape(GRID_B, GRID_Z, 2, SHARED_B)
    band_lists = shuffled[:, 2 * SHARED_B:2 * SHARED_B + 2 * SHARED_Z].reshape(GRID_B, GRID_Z, 2, SHARED_Z)
    return (counts, blk_lists, band_lists)


def draw_halo_count(key, part):
    return halo_plan(key)[0]


def draw_blk_nodes(key, part):
    return halo_plan(key)[1]


def draw_band_nodes(key, part):
    return halo_plan(key)[2]


def with_ends(entries, stream_key, low, high):
    shape = entries.shape
    index_at = [jax.random.randint(jax.random.fold_in(stream_key, axis), (), 0, shape[axis]) for axis in range(len(shape))]
    entries = entries.at[tuple(index_at)].set(low)
    longest = shape.index(max(shape))
    index_at[longest] = (index_at[longest] + 1) % shape[longest]
    return entries.at[tuple(index_at)].set(high)


def shard_levels(key, shape, shards, low, top_value):
    def one(dim, blocks):
        heights = jax.random.uniform(jax.random.fold_in(jax.random.fold_in(key, 6), dim), (blocks,), jnp.float32, low / len(shards), top_value / len(shards))
        return jnp.repeat(jnp.exp(heights), shape[dim] // blocks).reshape((-1,) + (1,) * (len(shape) - dim - 1))

    gain = one(*shards[0])
    for cut in shards[1:]:
        gain = gain * one(*cut)
    return gain


def cumulative_ranks(amount, slope):
    loads = [(1 << 20) // math.isqrt(rank ** slope) + 1 for rank in range(1, amount + 1)]
    spread = 1 + sum(loads) // (1 << 30)
    return np.cumsum(np.array([max(1, weight // spread) for weight in loads]))


def ranked(rng, dims, count, slope):
    grid = cumulative_ranks(count, slope)
    lot = jax.random.randint(jax.random.fold_in(rng, 1), dims, 0, int(grid[count - 1]))
    rank = jnp.searchsorted(jnp.asarray(grid, jnp.int32), lot, side="right")
    return jax.random.permutation(jax.random.fold_in(rng, 2), count)[rank].astype(jnp.int32)


def scatter_about(own_key, extent, scale, limit, cuts=(), kind=jnp.bfloat16):
    entries = scale * jax.random.normal(own_key, extent, jnp.float32)
    if cuts:
        entries = entries * shard_levels(own_key, extent, cuts, -0.22, 0.18)
    return jnp.clip(entries, -limit, limit).astype(kind)


def setup_inputs(seed: int = 0) -> dict:
    splits = jax.random.split(jax.random.key(seed), 13)
    disp_fwd = scatter_about(splits[0], (GRID_B, DEPTH, NODES, COEFF), 1.0, 6.0, ((0, 16), (1, 2)), jnp.float32)
    prev_fwd = scatter_about(splits[1], (GRID_B, DEPTH, NODES, COEFF), 1.0, 6.0, ((0, 16), (1, 2)), jnp.float32)
    disp_adj = scatter_about(splits[2], (GRID_B, DEPTH, NODES, COEFF), 1.0, 6.0, ((0, 16), (1, 2)), jnp.float32)
    prev_adj = scatter_about(splits[3], (GRID_B, DEPTH, NODES, COEFF), 1.0, 6.0, ((0, 16), (1, 2)), jnp.float32)
    modulus = jnp.clip(jnp.exp(math.log(2.0) - 1.3862944 * jax.random.uniform(splits[4], (GRID_B, DEPTH, NODES, SAMPLES), jnp.float32) ** shard_levels(splits[4], (GRID_B, DEPTH, NODES, SAMPLES), ((0, 16), (1, 2)), -0.2, 0.2)), 0.5, 2.0)
    radius = jnp.clip(jnp.exp(math.log(2048.0) - 2.0794415 * jax.random.uniform(splits[5], (GRID_B, DEPTH, NODES), jnp.float32) ** shard_levels(splits[5], (GRID_B, DEPTH, NODES), ((0, 16), (1, 2)), -0.2, 0.2)), 256.0, 2048.0)
    step_scale = jnp.clip(jnp.exp(math.log(0.04) - 1.3862944 * jax.random.uniform(splits[6], (GRID_B, DEPTH, NODES), jnp.float32) ** shard_levels(splits[6], (GRID_B, DEPTH, NODES), ((0, 16), (1, 2)), -0.2, 0.2)), 0.01, 0.04)
    kernel_in = scatter_about(splits[7], (GRID_B, DEPTH, NODES, SAMPLES), 1.0, 6.0, ((0, 16), (1, 2)), jnp.float32)
    buckets = with_ends(ranked(splits[8], (GRID_B, DEPTH), 4, 2), jax.random.fold_in(splits[8], 3), 0, 3).astype(jnp.int32)
    halo_count = draw_halo_count(jax.random.fold_in(splits[12], 71), 0)
    blk_nodes = draw_blk_nodes(jax.random.fold_in(splits[12], 71), 0)
    band_nodes = draw_band_nodes(jax.random.fold_in(splits[12], 71), 0)
    return dict(disp_fwd=disp_fwd, prev_fwd=prev_fwd, disp_adj=disp_adj, prev_adj=prev_adj, modulus=modulus, radius=radius, step_scale=step_scale, kernel_in=kernel_in, buckets=buckets, halo_count=halo_count, blk_nodes=blk_nodes, band_nodes=band_nodes)


def gll_tables():
    inner_root = math.sqrt(3.0 / 7.0)
    points = np.array([-1.0, -inner_root, 0.0, inner_root, 1.0])
    weights = np.array([0.1, 49.0 / 90.0, 32.0 / 45.0, 49.0 / 90.0, 0.1])
    legendre = (35.0 * points ** 4 - 30.0 * points ** 2 + 3.0) / 8.0
    derivative = np.zeros((5, 5))
    for target in range(5):
        for source in range(5):
            if target != source:
                derivative[target, source] = legendre[target] / legendre[source] / (points[target] - points[source])
    derivative[0, 0] = -5.0
    derivative[4, 4] = 5.0
    return (jnp.asarray(derivative, jnp.float32), jnp.asarray(np.outer(weights, weights), jnp.float32))

def azimuth_table(mode_total):
    sample_len = 2 * mode_total
    table_shape = (2 * mode_total, sample_len)
    row_ids = lax.broadcasted_iota(jnp.int32, table_shape, 0)
    col_ids = lax.broadcasted_iota(jnp.int32, table_shape, 1)
    quarter = (row_ids >= mode_total).astype(jnp.int32) * (sample_len // 4)
    phase = (row_ids % mode_total * col_ids + quarter) % sample_len
    factor = math.sqrt(2.0 / sample_len)
    return (jnp.cos(phase.astype(jnp.float32) * (2.0 * math.pi / sample_len)) * factor).astype(jnp.bfloat16)

def mode_tops(mode_total):
    return [max(mode_total // 64, 1), max(mode_total // 16, 1), max(mode_total // 4, 1), mode_total]

def mode_mask(buckets, mode_total):
    order_tops = mode_tops(mode_total)
    order_limit = jnp.where(buckets == 0, order_tops[0], jnp.where(buckets == 1, order_tops[1], jnp.where(buckets == 2, order_tops[2], order_tops[3])))
    kept = (jnp.arange(mode_total, dtype=jnp.int32) < order_limit[..., None]).astype(jnp.float32)
    return jnp.concatenate([kept, kept], axis=-1)

def spin(coeffs, inv_radius, mode_orders):
    half_len = mode_orders.shape[0]
    return jnp.concatenate([-mode_orders * coeffs[..., half_len:], mode_orders * coeffs[..., :half_len]], axis=-1) * inv_radius

def unspin(coeffs, inv_radius, mode_orders):
    half_len = mode_orders.shape[0]
    return jnp.concatenate([mode_orders * coeffs[..., half_len:], -mode_orders * coeffs[..., :half_len]], axis=-1) * inv_radius

def field_terms(coeffs, inv_radius, weight, azim_table, derivative):
    element_total = coeffs.shape[0]
    coeff_len = coeffs.shape[-1]
    sample_len = azim_table.shape[1]
    mode_orders = jnp.arange(coeff_len // 2, dtype=jnp.float32)
    physical = jnp.dot(coeffs.astype(jnp.bfloat16).reshape(-1, coeff_len), azim_table, preferred_element_type=jnp.float32).reshape(element_total, 5, 5, sample_len)
    spun_low = spin(coeffs, inv_radius, mode_orders).astype(jnp.bfloat16).reshape(-1, coeff_len)
    azimuthal = jnp.dot(spun_low, azim_table, preferred_element_type=jnp.float32).reshape(element_total, 5, 5, sample_len)
    grad_s = jnp.einsum('ab,ebjk->eajk', derivative, physical, precision=lax.Precision.HIGHEST)
    grad_z = jnp.einsum('ab,eibk->eiak', derivative, physical, precision=lax.Precision.HIGHEST)
    diverge = jnp.einsum('ba,ebjk->eajk', derivative, weight * grad_s, precision=lax.Precision.HIGHEST) + jnp.einsum('ba,eibk->eiak', derivative, weight * grad_z, precision=lax.Precision.HIGHEST)
    contract_dims = (((1,), (1,)), ((), ()))
    back_div = lax.dot_general(diverge.astype(jnp.bfloat16).reshape(-1, sample_len), azim_table, contract_dims, preferred_element_type=jnp.float32).reshape(element_total, 25, coeff_len)
    back_phi = lax.dot_general((weight * azimuthal).astype(jnp.bfloat16).reshape(-1, sample_len), azim_table, contract_dims, preferred_element_type=jnp.float32).reshape(element_total, 25, coeff_len)
    stiff = back_div + unspin(back_phi, inv_radius, mode_orders)
    return (stiff, grad_s, grad_z, azimuthal)

def pick_rows(table, nodes):
    return table[nodes]

def add_rows(target, nodes, values):
    return target.at[nodes].add(values)

def reference(disp_fwd, prev_fwd, disp_adj, prev_adj, modulus, radius, step_scale, kernel_in, buckets, halo_count, blk_nodes, band_nodes):
    derivative, quadrature = gll_tables()
    azim_table = azimuth_table(MODES)

    def column(inputs):
        col_fwd, col_adj, col_mod, col_rad, col_bucket, col_kernel = inputs
        kept = mode_mask(col_bucket, MODES)[:, None, :]
        inv_radius = 1.0 / col_rad[..., None]
        weight = col_mod.reshape(-1, 5, 5, SAMPLES) * quadrature[None, :, :, None]
        stiff_fwd, fwd_s, fwd_z, fwd_p = field_terms(col_fwd * kept, inv_radius, weight, azim_table, derivative)
        stiff_adj, adj_s, adj_z, adj_p = field_terms(col_adj * kept, inv_radius, weight, azim_table, derivative)
        products = fwd_s * adj_s + fwd_z * adj_z + fwd_p * adj_p
        kernel = col_kernel - (quadrature[None, :, :, None] * products).reshape(-1, NODES, SAMPLES)
        return (stiff_fwd * kept, stiff_adj * kept, kernel)
    stiff_fwd, stiff_adj, kernel_out = lax.map(column, (disp_fwd, disp_adj, modulus, radius, buckets, kernel_in))

    def assemble(stiff):
        local = stiff.reshape(GRID_B, GRID_Z, EL_DEV * NODES, COEFF)
        picker = jax.vmap(jax.vmap(pick_rows))
        placer = jax.vmap(jax.vmap(add_rows))
        blk_slots = jnp.arange(SHARED_B, dtype=jnp.int32)
        band_slots = jnp.arange(SHARED_Z, dtype=jnp.int32)
        total = local
        sends = picker(local, blk_nodes[:, :, 1])
        arrived = jnp.concatenate([jnp.zeros_like(sends[:1]), sends[:-1]], axis=0)
        valid = (blk_slots[None, None, :] < halo_count[:, :, 0:1]).astype(jnp.float32)[..., None]
        total = placer(total, blk_nodes[:, :, 0], arrived * valid)
        sends = picker(local, blk_nodes[:, :, 0])
        arrived = jnp.concatenate([sends[1:], jnp.zeros_like(sends[:1])], axis=0)
        valid = (blk_slots[None, None, :] < halo_count[:, :, 1:2]).astype(jnp.float32)[..., None]
        total = placer(total, blk_nodes[:, :, 1], arrived * valid)
        sends = picker(local, band_nodes[:, :, 1])
        arrived = jnp.concatenate([jnp.zeros_like(sends[:, :1]), sends[:, :-1]], axis=1)
        valid = (band_slots[None, None, :] < halo_count[:, :, 2:3]).astype(jnp.float32)[..., None]
        total = placer(total, band_nodes[:, :, 0], arrived * valid)
        sends = picker(local, band_nodes[:, :, 0])
        arrived = jnp.concatenate([sends[:, 1:], jnp.zeros_like(sends[:, :1])], axis=1)
        valid = (band_slots[None, None, :] < halo_count[:, :, 3:4]).astype(jnp.float32)[..., None]
        total = placer(total, band_nodes[:, :, 1], arrived * valid)
        return total.reshape(GRID_B, DEPTH, NODES, COEFF)
    kept_all = mode_mask(buckets, MODES)[:, :, None, :]
    growth = step_scale[..., None]
    next_fwd = kept_all * (2.0 * (disp_fwd * kept_all) - prev_fwd - growth * assemble(stiff_fwd))
    next_adj = kept_all * (2.0 * (disp_adj * kept_all) - prev_adj - growth * assemble(stiff_adj))
    return (next_fwd, next_adj, kernel_out)
```

```python
import functools
import math

import jax
import jax.numpy as jnp
import ml_dtypes
import numpy as np
from jax import lax
from jax.experimental import pallas as pl
from jax.experimental.pallas import tpu as pltpu
from jax.sharding import PartitionSpec as P

MESH = pl.DeviceIdType.MESH


def gll_tables():
    inner_root = math.sqrt(3.0 / 7.0)
    points = np.array([-1.0, -inner_root, 0.0, inner_root, 1.0])
    weights = np.array([0.1, 49.0 / 90.0, 32.0 / 45.0, 49.0 / 90.0, 0.1])
    legendre = (35.0 * points**4 - 30.0 * points**2 + 3.0) / 8.0
    derivative = np.zeros((5, 5))
    for target in range(5):
        for source in range(5):
            if target != source:
                derivative[target, source] = (
                    legendre[target] / legendre[source] / (points[target] - points[source])
                )
    derivative[0, 0] = -5.0
    derivative[4, 4] = 5.0
    return derivative.astype(np.float32), np.outer(weights, weights).astype(np.float32)


def half_table(mode_total, width):
    sample_len = 2 * mode_total
    rows = np.arange(2 * mode_total, dtype=np.int64)
    quarter = (rows >= mode_total) * (sample_len // 4)
    phase = ((rows % mode_total)[:, None] * np.arange(mode_total)[None] + quarter[:, None]) % sample_len
    levels = np.cos(np.arange(sample_len) * (2.0 * math.pi / sample_len)) * math.sqrt(2.0 / sample_len)
    levels = levels.astype(np.float32).astype(ml_dtypes.bfloat16)
    table = levels[phase]
    return table.reshape(2 * mode_total, mode_total // width, width).transpose(1, 0, 2)


def split_bf16(value):
    high = value.astype(np.float32).astype(ml_dtypes.bfloat16)
    low = (value.astype(np.float32) - high.astype(np.float32)).astype(ml_dtypes.bfloat16)
    return high, low


def node_operators(pad):
    derivative, quadrature = gll_tables()
    eye = np.eye(5, dtype=np.float32)
    along_s = np.zeros((pad, pad), np.float32)
    along_z = np.zeros((pad, pad), np.float32)
    along_s[:25, :25] = np.kron(derivative, eye)
    along_z[:25, :25] = np.kron(eye, derivative)
    grad_hi, grad_lo = split_bf16(np.concatenate([along_s, along_z], axis=0))
    div_hi, div_lo = split_bf16(np.concatenate([along_s.T, along_z.T], axis=1))
    quad = np.zeros((pad, 128), np.float32)
    quad[:25] = quadrature.reshape(25, 1)
    return (
        np.concatenate([grad_hi, grad_hi, grad_lo], axis=1),
        np.concatenate([div_hi, div_hi, div_lo], axis=1),
        quad,
    )


def halves(value):
    high = value.astype(jnp.bfloat16)
    low = (value - high.astype(jnp.float32)).astype(jnp.bfloat16)
    return high, low


def mm(lhs, rhs):
    return jnp.dot(lhs, rhs, preferred_element_type=jnp.float32)


def padded(value, pad):
    extra = pad - value.shape[0]
    return jnp.concatenate([value, jnp.zeros((extra, value.shape[1]), value.dtype)], axis=0)


def column_of(row, pad):
    count = row.shape[1]
    sub = lax.broadcasted_iota(jnp.int32, (pad, count), 0)
    lane = lax.broadcasted_iota(jnp.int32, (pad, count), 1)
    return jnp.sum(jnp.where(sub == lane, row, 0.0), axis=1, keepdims=True)


def kernel(
    blk_total,
    band_total,
    nodes,
    pad,
    width,
    disp_fwd,
    prev_fwd,
    disp_adj,
    prev_adj,
    modulus,
    kernel_in,
    radius,
    step_scale,
    grad_op,
    div_op,
    quad,
    bucket,
    counts,
    blk_nodes,
    band_nodes,
    table_hbm,
    next_fwd,
    next_adj,
    kernel_out,
    table,
    rows,
    low,
    stiff,
    send_blk,
    send_band,
    recv_blk,
    recv_band,
    table_sem,
    send_sem,
    recv_sem,
):
    blk = lax.axis_index("blk")
    band = lax.axis_index("band")
    half = disp_fwd.shape[-1] // 2
    chunks = half // width
    blk_slots = blk_nodes.shape[-1]
    band_slots = band_nodes.shape[-1]
    links = [
        (blk > 0, (blk - 1, band)),
        (blk < blk_total - 1, (blk + 1, band)),
        (band > 0, (blk, band - 1)),
        (band < band_total - 1, (blk, band + 1)),
    ]
    loads = [
        pltpu.make_async_copy(table_hbm.at[c], table.at[c], table_sem.at[c]) for c in range(chunks)
    ]
    for load in loads:
        load.start()
    barrier = pltpu.get_barrier_semaphore()
    for here, peer in links:

        @pl.when(here)
        def _():
            pl.semaphore_signal(barrier, inc=1, device_id=peer, device_id_type=MESH)

    def landing(c, side):
        return recv_blk.at[c, side] if side < 2 else recv_band.at[c, side - 2]

    def leaving(c, side):
        return send_blk.at[c, side] if side < 2 else send_band.at[c, side - 2]

    def transfer(c, side):
        return pltpu.make_async_remote_copy(
            src_ref=leaving(c, side),
            dst_ref=landing(c, side ^ 1),
            send_sem=send_sem.at[c, side],
            recv_sem=recv_sem.at[c, side ^ 1],
            device_id=links[side][1],
            device_id_type=MESH,
        )

    def arrival(c, side):
        return pltpu.make_async_remote_copy(
            src_ref=leaving(c, side),
            dst_ref=landing(c, side),
            send_sem=send_sem.at[c, side],
            recv_sem=recv_sem.at[c, side],
            device_id=links[side][1],
            device_id_type=MESH,
        )

    for side in range(4):

        @pl.when(jnp.logical_not(links[side][0]))
        def _():
            for c in range(chunks):
                ref = landing(c, side)
                ref[...] = jnp.zeros(ref.shape, ref.dtype)

    level = bucket[0, 0]
    tops = [max(half // 64, 1), max(half // 16, 1), max(half // 4, 1), half]
    limit = jnp.where(
        level == 0, tops[0], jnp.where(level == 1, tops[1], jnp.where(level == 2, tops[2], tops[3]))
    )
    radius_col = column_of(radius[0], pad)
    sub_col = lax.broadcasted_iota(jnp.int32, (pad, 1), 0)
    inv_radius = jnp.where(sub_col < nodes, 1.0 / radius_col, 0.0)
    growth = column_of(step_scale[0], pad)
    quad_col = quad[:, 0:1]
    fields = ((disp_fwd, prev_fwd, next_fwd), (disp_adj, prev_adj, next_adj))

    def orders(c):
        m = lax.broadcasted_iota(jnp.int32, (1, width), 1) + c * width
        kept = (m < limit).astype(jnp.float32)
        sign = (1 - 2 * (m % 2)).astype(jnp.float32)
        return m.astype(jnp.float32), kept, sign

    for f, (disp, _, _) in enumerate(fields):
        for c in range(chunks):
            m, kept, sign = orders(c)
            re_cols = slice(c * width, (c + 1) * width)
            im_cols = slice(half + c * width, half + (c + 1) * width)
            real = padded(disp[0, 0, :, re_cols], pad) * kept
            imag = padded(disp[0, 0, :, im_cols], pad) * kept
            spin_re = -m * imag * inv_radius
            spin_im = m * real * inv_radius
            for k, (re_part, im_part) in enumerate(((real, imag), (spin_re, spin_im))):
                at = (4 * f + 2 * k) * pad
                rows[at : at + pad, re_cols] = re_part.astype(jnp.bfloat16)
                rows[at : at + pad, im_cols] = im_part.astype(jnp.bfloat16)
                rows[at + pad : at + 2 * pad, re_cols] = (re_part * sign).astype(jnp.bfloat16)
                rows[at + pad : at + 2 * pad, im_cols] = (im_part * sign).astype(jnp.bfloat16)

    for c in range(chunks):
        loads[c].wait()
        samples = mm(rows[...], table[c])
        chunk_cols = slice(c * width, (c + 1) * width)
        for h in range(2):
            cols = slice(h * half + c * width, h * half + (c + 1) * width)
            weight = padded(modulus[0, 0, :, cols], pad) * quad_col
            terms = []
            for f in range(2):
                at = (4 * f + h) * pad
                physical = samples[at : at + pad]
                azimuthal = samples[at + 2 * pad : at + 3 * pad]
                high, lower = halves(physical)
                grads = mm(grad_op[...], jnp.concatenate([high, lower, high], axis=0))
                grad_s, grad_z = grads[:pad], grads[pad:]
                high_s, low_s = halves(weight * grad_s)
                high_z, low_z = halves(weight * grad_z)
                diverge = mm(
                    div_op[...],
                    jnp.concatenate([high_s, high_z, low_s, low_z, high_s, high_z], axis=0),
                )
                low[at : at + pad, chunk_cols] = diverge.astype(jnp.bfloat16)
                low[at + 2 * pad : at + 3 * pad, chunk_cols] = (weight * azimuthal).astype(
                    jnp.bfloat16
                )
                terms.append((grad_s, grad_z, azimuthal))
            product = sum(one * two for one, two in zip(*terms))
            kernel_out[0, 0, :, cols] = kernel_in[0, 0, :, cols] - (quad_col * product)[:nodes]

    pl.semaphore_wait(barrier, sum(here.astype(jnp.int32) for here, _ in links))

    for c in range(chunks):
        m, kept, sign = orders(c)
        cosines = mm(low[...], table[c, :half])
        sines = mm(low[...], table[c, half:])

        def joined(result, group):
            at = group * pad
            return result[at : at + pad] + sign * result[at + pad : at + 2 * pad]

        for f in range(2):
            real = kept * (joined(cosines, 4 * f) + m * joined(sines, 4 * f + 2) * inv_radius)
            imag = kept * (joined(sines, 4 * f) - m * joined(cosines, 4 * f + 2) * inv_radius)
            stiff[c, f, :, :width] = real
            stiff[c, f, :, width:] = imag
        for side in range(2):
            for f in range(2):
                for s in range(blk_slots):
                    node = blk_nodes[0, 0, side, s]
                    at = f * blk_slots + s
                    send_blk[c, side, at : at + 1, :] = stiff[c, f, pl.ds(node, 1), :]
                for s in range(band_slots):
                    node = band_nodes[0, 0, side, s]
                    at = f * band_slots + s
                    send_band[c, side, at : at + 1, :] = stiff[c, f, pl.ds(node, 1), :]
        for side in range(4):

            @pl.when(links[side][0])
            def _():
                transfer(c, side).start()

    slot_rows = 4 * (blk_slots + band_slots)
    lane = lax.broadcasted_iota(jnp.int32, (1, 2 * slot_rows), 1) % slot_rows
    target = jnp.full((1, 2 * slot_rows), -1, jnp.int32)
    at = 0
    for side in range(4):
        lists = blk_nodes if side < 2 else band_nodes
        for f in range(2):
            for s in range(lists.shape[-1]):
                node = jnp.where(s < counts[0, 0, side], lists[0, 0, side % 2, s] + f * pad, -1)
                target = jnp.where(lane == at, node, target)
                at += 1
    sub = lax.broadcasted_iota(jnp.int32, (2 * pad, 2 * slot_rows), 0)
    placer = jnp.where(sub == target, 1.0, 0.0).astype(jnp.bfloat16)

    for c in range(chunks):
        for side in range(4):

            @pl.when(links[side][0])
            def _():
                arrival(c, side).wait_recv()

        m, kept, _ = orders(c)
        arrived = jnp.concatenate([landing(c, side)[...] for side in range(4)], axis=0)
        high, lower = halves(arrived)
        placed = mm(placer, jnp.concatenate([high, lower], axis=0))
        for f, (disp, prev, out) in enumerate(fields):
            for part in range(2):
                cols = slice(part * half + c * width, part * half + (c + 1) * width)
                sect = slice(part * width, (part + 1) * width)
                total = stiff[c, f, :, sect] + placed[f * pad : (f + 1) * pad, sect]
                out[0, 0, :, cols] = kept * (
                    2.0 * disp[0, 0, :, cols] - prev[0, 0, :, cols] - (growth * total)[:nodes]
                )
    for c in range(chunks):
        for side in range(4):

            @pl.when(links[side][0])
            def _():
                transfer(c, side).wait_send()


def per_device(
    blk_total,
    band_total,
    disp_fwd,
    prev_fwd,
    disp_adj,
    prev_adj,
    modulus,
    radius,
    step_scale,
    kernel_in,
    buckets,
    halo_count,
    blk_nodes,
    band_nodes,
):
    nodes, coeff_len = disp_fwd.shape[2:]
    half = coeff_len // 2
    width = min(512, half)
    chunks = half // width
    pad = -(-nodes // 16) * 16
    blk_slots = blk_nodes.shape[-1]
    band_slots = band_nodes.shape[-1]
    grad_op, div_op, quad = node_operators(pad)
    table = half_table(half, width)
    vmem = pl.BlockSpec(memory_space=pltpu.VMEM)
    smem = pl.BlockSpec(memory_space=pltpu.SMEM)
    out = jax.ShapeDtypeStruct(disp_fwd.shape, jnp.float32)
    return pl.pallas_call(
        functools.partial(kernel, blk_total, band_total, nodes, pad, width),
        out_shape=(out, out, out),
        in_specs=[vmem] * 11 + [smem] * 4 + [pl.BlockSpec(memory_space=pltpu.HBM)],
        out_specs=(vmem, vmem, vmem),
        scratch_shapes=[
            pltpu.VMEM(table.shape, jnp.bfloat16),
            pltpu.VMEM((8 * pad, coeff_len), jnp.bfloat16),
            pltpu.VMEM((8 * pad, half), jnp.bfloat16),
            pltpu.VMEM((chunks, 2, pad, 2 * width), jnp.float32),
            pltpu.VMEM((chunks, 2, 2 * blk_slots, 2 * width), jnp.float32),
            pltpu.VMEM((chunks, 2, 2 * band_slots, 2 * width), jnp.float32),
            pltpu.VMEM((chunks, 2, 2 * blk_slots, 2 * width), jnp.float32),
            pltpu.VMEM((chunks, 2, 2 * band_slots, 2 * width), jnp.float32),
            pltpu.SemaphoreType.DMA((chunks,)),
            pltpu.SemaphoreType.DMA((chunks, 4)),
            pltpu.SemaphoreType.DMA((chunks, 4)),
        ],
        compiler_params=pltpu.CompilerParams(
            collective_id=0, has_side_effects=True, vmem_limit_bytes=60 * 1024 * 1024
        ),
    )(
        disp_fwd,
        prev_fwd,
        disp_adj,
        prev_adj,
        modulus,
        kernel_in,
        radius,
        step_scale,
        jnp.asarray(grad_op),
        jnp.asarray(div_op),
        jnp.asarray(quad),
        buckets,
        halo_count,
        blk_nodes,
        band_nodes,
        jnp.asarray(table),
    )


def solution(mesh):
    wide = P("blk", "band", None, None)
    line = P("blk", "band", None)
    in_specs = (wide,) * 5 + (line, line, wide, P("blk", "band"), line, wide, wide)
    return jax.shard_map(
        functools.partial(per_device, mesh.shape["blk"], mesh.shape["band"]),
        mesh=mesh,
        in_specs=in_specs,
        out_specs=(wide,) * 3,
        check_vma=False,
    )
```

```python
import functools
import math

import jax
import jax.numpy as jnp
import ml_dtypes
import numpy as np
from jax import lax
from jax.experimental import pallas as pl
from jax.experimental.pallas import tpu as pltpu
from jax.sharding import PartitionSpec as P

MESH = pl.DeviceIdType.MESH


def gll_tables():
    inner_root = math.sqrt(3.0 / 7.0)
    points = np.array([-1.0, -inner_root, 0.0, inner_root, 1.0])
    weights = np.array([0.1, 49.0 / 90.0, 32.0 / 45.0, 49.0 / 90.0, 0.1])
    legendre = (35.0 * points**4 - 30.0 * points**2 + 3.0) / 8.0
    derivative = np.zeros((5, 5))
    for target in range(5):
        for source in range(5):
            if target != source:
                derivative[target, source] = (
                    legendre[target] / legendre[source] / (points[target] - points[source])
                )
    derivative[0, 0] = -5.0
    derivative[4, 4] = 5.0
    return derivative.astype(np.float32), np.outer(weights, weights).astype(np.float32)


def half_table(mode_total, width):
    sample_len = 2 * mode_total
    rows = np.arange(2 * mode_total, dtype=np.int64)
    quarter = (rows >= mode_total) * (sample_len // 4)
    phase = ((rows % mode_total)[:, None] * np.arange(mode_total)[None] + quarter[:, None]) % sample_len
    levels = np.cos(np.arange(sample_len) * (2.0 * math.pi / sample_len)) * math.sqrt(2.0 / sample_len)
    levels = levels.astype(np.float32).astype(ml_dtypes.bfloat16)
    table = levels[phase]
    return table.reshape(2 * mode_total, mode_total // width, width).transpose(1, 0, 2)


def split_bf16(value):
    high = value.astype(np.float32).astype(ml_dtypes.bfloat16)
    low = (value.astype(np.float32) - high.astype(np.float32)).astype(ml_dtypes.bfloat16)
    return high, low


def node_operators(pad):
    derivative, quadrature = gll_tables()
    eye = np.eye(5, dtype=np.float32)
    along_s = np.zeros((pad, pad), np.float32)
    along_z = np.zeros((pad, pad), np.float32)
    along_s[:25, :25] = np.kron(derivative, eye)
    along_z[:25, :25] = np.kron(eye, derivative)
    grad_hi, grad_lo = split_bf16(np.concatenate([along_s, along_z], axis=0))
    div_hi, div_lo = split_bf16(np.concatenate([along_s.T, along_z.T], axis=1))
    quad = np.zeros((pad, 128), np.float32)
    quad[:25] = quadrature.reshape(25, 1)
    return (
        np.concatenate([grad_hi, grad_hi, grad_lo], axis=1),
        np.concatenate([div_hi, div_hi, div_lo], axis=1),
        quad,
    )


def halves(value):
    high = value.astype(jnp.bfloat16)
    low = (value - high.astype(jnp.float32)).astype(jnp.bfloat16)
    return high, low


def mm(lhs, rhs):
    return jnp.dot(lhs, rhs, preferred_element_type=jnp.float32)


def padded(value, pad):
    extra = pad - value.shape[0]
    return jnp.concatenate([value, jnp.zeros((extra, value.shape[1]), value.dtype)], axis=0)


def take(ref, nodes, start, size):
    stride = ref.shape[0] // nodes
    return jnp.concatenate(
        [ref[pl.ds(start // 128 + j, nodes, stride=stride), :] for j in range(size // 128)], axis=1
    )


def put(ref, nodes, start, value):
    stride = ref.shape[0] // nodes
    for j in range(value.shape[1] // 128):
        ref[pl.ds(start // 128 + j, nodes, stride=stride), :] = value[:, j * 128 : (j + 1) * 128]


def column_of(row, pad):
    count = row.shape[1]
    sub = lax.broadcasted_iota(jnp.int32, (pad, count), 0)
    lane = lax.broadcasted_iota(jnp.int32, (pad, count), 1)
    return jnp.sum(jnp.where(sub == lane, row, 0.0), axis=1, keepdims=True)


def kernel(
    blk_total,
    band_total,
    nodes,
    pad,
    width,
    disp_fwd_hbm,
    prev_fwd_hbm,
    disp_adj_hbm,
    prev_adj_hbm,
    modulus_hbm,
    kernel_in_hbm,
    radius_hbm,
    step_hbm,
    bucket_hbm,
    grad_hbm,
    div_hbm,
    quad_hbm,
    counts_hbm,
    blk_nodes_hbm,
    band_nodes_hbm,
    table_hbm,
    next_fwd,
    next_adj,
    kernel_out,
    held,
    radius,
    step_scale,
    bucket,
    grad_op,
    div_op,
    quad,
    counts,
    blk_nodes,
    band_nodes,
    table,
    rows,
    low,
    stiff,
    send_blk,
    send_band,
    recv_blk,
    recv_band,
    held_sem,
    small_sem,
    table_sem,
    send_sem,
    recv_sem,
):
    disp_fwd, disp_adj, modulus, kernel_in, prev_fwd, prev_adj = (held.at[i] for i in range(6))
    sources = (disp_fwd_hbm, disp_adj_hbm, modulus_hbm, kernel_in_hbm, prev_fwd_hbm, prev_adj_hbm)
    fetches = [
        pltpu.make_async_copy(source, held.at[i], held_sem.at[i])
        for i, source in enumerate(sources)
    ]
    small = [
        pltpu.make_async_copy(source, target, small_sem.at[i])
        for i, (source, target) in enumerate(
            (
                (radius_hbm, radius),
                (step_hbm, step_scale),
                (bucket_hbm, bucket),
                (grad_hbm, grad_op),
                (div_hbm, div_op),
                (quad_hbm, quad),
                (counts_hbm, counts),
                (blk_nodes_hbm, blk_nodes),
                (band_nodes_hbm, band_nodes),
            )
        )
    ]
    fetches[0].start()
    for copy in small:
        copy.start()
    fetches[1].start()
    blk = lax.axis_index("blk")
    band = lax.axis_index("band")
    half = disp_fwd_hbm.shape[0] // nodes * 128 // 2
    chunks = half // width
    blk_slots = blk_nodes.shape[-1]
    band_slots = band_nodes.shape[-1]
    links = [
        (blk > 0, (blk - 1, band)),
        (blk < blk_total - 1, (blk + 1, band)),
        (band > 0, (blk, band - 1)),
        (band < band_total - 1, (blk, band + 1)),
    ]
    loads = [
        pltpu.make_async_copy(table_hbm.at[c], table.at[c], table_sem.at[c]) for c in range(chunks)
    ]
    for load in loads:
        load.start()
    for fetch in fetches[2:]:
        fetch.start()
    barrier = pltpu.get_barrier_semaphore()
    for here, peer in links:

        @pl.when(here)
        def _():
            pl.semaphore_signal(barrier, inc=1, device_id=peer, device_id_type=MESH)

    def landing(c, side):
        return recv_blk.at[c, side] if side < 2 else recv_band.at[c, side - 2]

    def leaving(c, side):
        return send_blk.at[c, side] if side < 2 else send_band.at[c, side - 2]

    def transfer(c, side):
        return pltpu.make_async_remote_copy(
            src_ref=leaving(c, side),
            dst_ref=landing(c, side ^ 1),
            send_sem=send_sem.at[c, side],
            recv_sem=recv_sem.at[c, side ^ 1],
            device_id=links[side][1],
            device_id_type=MESH,
        )

    def arrival(c, side):
        return pltpu.make_async_remote_copy(
            src_ref=leaving(c, side),
            dst_ref=landing(c, side),
            send_sem=send_sem.at[c, side],
            recv_sem=recv_sem.at[c, side],
            device_id=links[side][1],
            device_id_type=MESH,
        )

    for side in range(4):

        @pl.when(jnp.logical_not(links[side][0]))
        def _():
            for c in range(chunks):
                ref = landing(c, side)
                ref[...] = jnp.zeros(ref.shape, ref.dtype)

    for copy in small:
        copy.wait()
    level = bucket[...]
    tops = [max(half // 64, 1), max(half // 16, 1), max(half // 4, 1), half]
    limit = jnp.where(
        level == 0, tops[0], jnp.where(level == 1, tops[1], jnp.where(level == 2, tops[2], tops[3]))
    )
    radius_col = column_of(radius[0], pad)
    sub_col = lax.broadcasted_iota(jnp.int32, (pad, 1), 0)
    inv_radius = jnp.where(sub_col < nodes, 1.0 / radius_col, 0.0)
    growth = column_of(step_scale[0], pad)
    quad_col = quad[:, 0:1]
    fields = ((disp_fwd, prev_fwd, next_fwd), (disp_adj, prev_adj, next_adj))

    def orders(c):
        m = lax.broadcasted_iota(jnp.int32, (1, width), 1) + c * width
        kept = (m < limit).astype(jnp.float32)
        sign = (1 - 2 * (m % 2)).astype(jnp.float32)
        return m.astype(jnp.float32), kept, sign

    for f, (disp, _, _) in enumerate(fields):
        fetches[f].wait()
        for c in range(chunks):
            m, kept, sign = orders(c)
            re_cols = slice(c * width, (c + 1) * width)
            im_cols = slice(half + c * width, half + (c + 1) * width)
            real = padded(take(disp, nodes, c * width, width), pad) * kept
            imag = padded(take(disp, nodes, half + c * width, width), pad) * kept
            spin_re = -m * imag * inv_radius
            spin_im = m * real * inv_radius
            for k, (re_part, im_part) in enumerate(((real, imag), (spin_re, spin_im))):
                at = (4 * f + 2 * k) * pad
                rows[at : at + pad, re_cols] = re_part.astype(jnp.bfloat16)
                rows[at : at + pad, im_cols] = im_part.astype(jnp.bfloat16)
                rows[at + pad : at + 2 * pad, re_cols] = (re_part * sign).astype(jnp.bfloat16)
                rows[at + pad : at + 2 * pad, im_cols] = (im_part * sign).astype(jnp.bfloat16)

    for c in range(chunks):
        loads[c].wait()
        if c == 0:
            fetches[2].wait()
            fetches[3].wait()
        samples = mm(rows[...], table[c])
        chunk_cols = slice(c * width, (c + 1) * width)
        for h in range(2):
            start = h * half + c * width
            weight = padded(take(modulus, nodes, start, width), pad) * quad_col
            terms = []
            for f in range(2):
                at = (4 * f + h) * pad
                physical = samples[at : at + pad]
                azimuthal = samples[at + 2 * pad : at + 3 * pad]
                high, lower = halves(physical)
                grads = mm(grad_op[...], jnp.concatenate([high, lower, high], axis=0))
                grad_s, grad_z = grads[:pad], grads[pad:]
                high_s, low_s = halves(weight * grad_s)
                high_z, low_z = halves(weight * grad_z)
                diverge = mm(
                    div_op[...],
                    jnp.concatenate([high_s, high_z, low_s, low_z, high_s, high_z], axis=0),
                )
                low[at : at + pad, chunk_cols] = diverge.astype(jnp.bfloat16)
                low[at + 2 * pad : at + 3 * pad, chunk_cols] = (weight * azimuthal).astype(
                    jnp.bfloat16
                )
                terms.append((grad_s, grad_z, azimuthal))
            product = sum(one * two for one, two in zip(*terms))
            change = (quad_col * product)[:nodes]
            put(kernel_out, nodes, start, take(kernel_in, nodes, start, width) - change)

    pl.semaphore_wait(barrier, sum(here.astype(jnp.int32) for here, _ in links))

    for c in range(chunks):
        m, kept, sign = orders(c)
        cosines = mm(low[...], table[c, :half])
        sines = mm(low[...], table[c, half:])

        def joined(result, group):
            at = group * pad
            return result[at : at + pad] + sign * result[at + pad : at + 2 * pad]

        for f in range(2):
            real = kept * (joined(cosines, 4 * f) + m * joined(sines, 4 * f + 2) * inv_radius)
            imag = kept * (joined(sines, 4 * f) - m * joined(cosines, 4 * f + 2) * inv_radius)
            stiff[c, f, :, :width] = real
            stiff[c, f, :, width:] = imag
        for side in range(2):
            for f in range(2):
                for s in range(blk_slots):
                    node = blk_nodes[0, 0, side, s]
                    at = f * blk_slots + s
                    send_blk[c, side, at : at + 1, :] = stiff[c, f, pl.ds(node, 1), :]
                for s in range(band_slots):
                    node = band_nodes[0, 0, side, s]
                    at = f * band_slots + s
                    send_band[c, side, at : at + 1, :] = stiff[c, f, pl.ds(node, 1), :]
        for side in range(4):

            @pl.when(links[side][0])
            def _():
                transfer(c, side).start()

    slot_rows = 4 * (blk_slots + band_slots)
    lane = lax.broadcasted_iota(jnp.int32, (1, 2 * slot_rows), 1) % slot_rows
    target = jnp.full((1, 2 * slot_rows), -1, jnp.int32)
    at = 0
    for side in range(4):
        lists = blk_nodes if side < 2 else band_nodes
        for f in range(2):
            for s in range(lists.shape[-1]):
                node = jnp.where(s < counts[0, 0, side], lists[0, 0, side % 2, s] + f * pad, -1)
                target = jnp.where(lane == at, node, target)
                at += 1
    sub = lax.broadcasted_iota(jnp.int32, (2 * pad, 2 * slot_rows), 0)
    placer = jnp.where(sub == target, 1.0, 0.0).astype(jnp.bfloat16)

    fetches[4].wait()
    fetches[5].wait()
    for c in range(chunks):
        for side in range(4):

            @pl.when(links[side][0])
            def _():
                arrival(c, side).wait_recv()

        m, kept, _ = orders(c)
        arrived = jnp.concatenate([landing(c, side)[...] for side in range(4)], axis=0)
        high, lower = halves(arrived)
        placed = mm(placer, jnp.concatenate([high, lower], axis=0))
        for f, (disp, prev, out) in enumerate(fields):
            for part in range(2):
                start = part * half + c * width
                now, before = (take(ref, nodes, start, width) for ref in (disp, prev))
                sect = slice(part * width, (part + 1) * width)
                total = stiff[c, f, :, sect] + placed[f * pad : (f + 1) * pad, sect]
                put(out, nodes, start, kept * (2.0 * now - before - (growth * total)[:nodes]))
    for c in range(chunks):
        for side in range(4):

            @pl.when(links[side][0])
            def _():
                transfer(c, side).wait_send()


def deliver(one, two, three, one_out, two_out, three_out, sems):
    copies = [
        pltpu.make_async_copy(source, target, sems.at[i])
        for i, (source, target) in enumerate(((one, one_out), (two, two_out), (three, three_out)))
    ]
    for copy in copies:
        copy.start()
    for copy in copies:
        copy.wait()


def per_device(
    blk_total,
    band_total,
    disp_fwd,
    prev_fwd,
    disp_adj,
    prev_adj,
    modulus,
    radius,
    step_scale,
    kernel_in,
    buckets,
    halo_count,
    blk_nodes,
    band_nodes,
):
    nodes, coeff_len = disp_fwd.shape[2:]
    half = coeff_len // 2
    width = min(512, half)
    chunks = half // width
    pad = -(-nodes // 16) * 16
    blk_slots = blk_nodes.shape[-1]
    band_slots = band_nodes.shape[-1]
    grad_op, div_op, quad = node_operators(pad)
    table = half_table(half, width)
    anywhere = pl.BlockSpec(memory_space=pl.ANY)
    hbm = pl.BlockSpec(memory_space=pltpu.HBM)
    flat = (nodes * coeff_len // 128, 128)
    out = jax.ShapeDtypeStruct(flat, jnp.float32)
    outs = pl.pallas_call(
        functools.partial(kernel, blk_total, band_total, nodes, pad, width),
        out_shape=(pltpu.VMEM(flat, jnp.float32),) * 3,
        in_specs=[hbm] * 16,
        out_specs=(pl.BlockSpec(memory_space=pltpu.VMEM),) * 3,
        scratch_shapes=[
            pltpu.VMEM((6, *flat), jnp.float32),
            pltpu.VMEM(radius.shape, jnp.float32),
            pltpu.VMEM(step_scale.shape, jnp.float32),
            pltpu.VMEM(buckets.shape, jnp.int32),
            pltpu.VMEM(grad_op.shape, jnp.bfloat16),
            pltpu.VMEM(div_op.shape, jnp.bfloat16),
            pltpu.VMEM(quad.shape, jnp.float32),
            pltpu.SMEM(halo_count.shape, jnp.int32),
            pltpu.SMEM(blk_nodes.shape, jnp.int32),
            pltpu.SMEM(band_nodes.shape, jnp.int32),
            pltpu.VMEM(table.shape, jnp.bfloat16),
            pltpu.VMEM((8 * pad, coeff_len), jnp.bfloat16),
            pltpu.VMEM((8 * pad, half), jnp.bfloat16),
            pltpu.VMEM((chunks, 2, pad, 2 * width), jnp.float32),
            pltpu.VMEM((chunks, 2, 2 * blk_slots, 2 * width), jnp.float32),
            pltpu.VMEM((chunks, 2, 2 * band_slots, 2 * width), jnp.float32),
            pltpu.VMEM((chunks, 2, 2 * blk_slots, 2 * width), jnp.float32),
            pltpu.VMEM((chunks, 2, 2 * band_slots, 2 * width), jnp.float32),
            pltpu.SemaphoreType.DMA((6,)),
            pltpu.SemaphoreType.DMA((9,)),
            pltpu.SemaphoreType.DMA((chunks,)),
            pltpu.SemaphoreType.DMA((chunks, 4)),
            pltpu.SemaphoreType.DMA((chunks, 4)),
        ],
        compiler_params=pltpu.CompilerParams(
            collective_id=0, has_side_effects=True, vmem_limit_bytes=67043328 - 3 * 4 * nodes * coeff_len - 40 * 1024
        ),
    )(
        disp_fwd.reshape(flat),
        prev_fwd.reshape(flat),
        disp_adj.reshape(flat),
        prev_adj.reshape(flat),
        modulus.reshape(flat),
        kernel_in.reshape(flat),
        radius,
        step_scale,
        buckets,
        jnp.asarray(grad_op),
        jnp.asarray(div_op),
        jnp.asarray(quad),
        halo_count,
        blk_nodes,
        band_nodes,
        jnp.asarray(table),
    )
    outs = pl.pallas_call(
        deliver,
        out_shape=(out, out, out),
        in_specs=[pl.BlockSpec(memory_space=pltpu.VMEM)] * 3,
        out_specs=(hbm,) * 3,
        scratch_shapes=[pltpu.SemaphoreType.DMA((3,))],
        compiler_params=pltpu.CompilerParams(vmem_limit_bytes=4 * 1024 * 1024),
    )(*outs)
    return tuple(value.reshape(disp_fwd.shape) for value in outs)


def solution(mesh):
    wide = P("blk", "band", None, None)
    line = P("blk", "band", None)
    in_specs = (wide,) * 5 + (line, line, wide, P("blk", "band"), line, wide, wide)
    return jax.shard_map(
        functools.partial(per_device, mesh.shape["blk"], mesh.shape["band"]),
        mesh=mesh,
        in_specs=in_specs,
        out_specs=(wide,) * 3,
        check_vma=False,
    )
```
